32 devices in a mesh: layer: 2 (over y), row: 4 (over x, core), col: 4 (over z).
Axes of the slice: x: 2, y: 2, z: 4, core: 2. Of those that a mesh axis runs over, the one named last changes fastest.
Arguments:
- ancestor: float32 [8192, 8192], P('row', 'col'), may hold values from -640 to 3200, as said below
- coupling: bfloat16 [2, 8192, 1024], P('layer', ('row', 'col')), may hold values from -10 to 10
- fronts: float32 [2, 2, 512, 512], P('layer', None, None, ('row', 'col')), may hold values from -10 to 360, as said below
- tile_pattern: int32 [2, 2, 8], P('layer'), may hold values 0 or 1
Outputs:
- schur: float32 [8192, 8192], P('row', 'col')
- panel_factor: float32 [8192, 512], P(('row', 'col'))
- pivots: float32 [512], P(('row', 'col'))
The draws below stay inside these ranges and needn't reach their ends.
Inputs may be any that keep to these rules, and one draw needn't show every extreme that they name: `ancestor`: symmetric and positive definite; the leading [512, 512] block of schur_0 stays positive definite after all layers' terms are subtracted. `fronts`: each [512, 512] block is symmetric and positive definite, with diagonal entries from 200 to 360 and other entries within -10 to 10.
All inputs are finite; a program needn't handle non-finite values. No bound on the sum of `tile_pattern` on one device may be relied on, other than what follows from the above.
Results may differ from the reference program's by a relative error of at most 0.0008.
Values may be sent and summed in bfloat16 or wider, within the bound.
No kernel may reach another device: no remote copies, remote signals or barrier semaphores. Data moves between devices by JAX's collectives and lax.ppermute only.
A program may use at most 128 MiB of HBM per device.

```python
import jax
import jax.numpy as jnp
from jax import lax

S = 8192
TILE = 1024
P_SIZE = 512
NP = 2
ANC = 1
LAYERS = 2
TILES = 8


def draw_ancestor(key, part):
    noise_key, factor_key, diag_key = jax.random.split(jax.random.fold_in(key, 11), 3)
    lowest = (S + LAYERS * NP * P_SIZE) / 8.0
    sample = jnp.clip(jax.random.normal(noise_key, (S, S), jnp.float32), -4.0, 4.0)
    factor = jax.random.normal(factor_key, (S, 2 * P_SIZE), jnp.float32)
    diagonal = jax.random.uniform(diag_key, (S,), jnp.float32, lowest, 1.25 * lowest)
    symmetric = jnp.clip((sample + sample.T) * 0.7071, -4.0, 4.0)
    coupled = jnp.dot(factor, factor.T, precision=lax.Precision.HIGHEST, preferred_element_type=jnp.float32)
    coupled = (coupled + coupled.T) * (0.5 * 0.75 * lowest / (2 * P_SIZE))
    is_diagonal = jnp.eye(S, dtype=bool)
    return jnp.where(is_diagonal, diagonal[:, None] + coupled, symmetric + coupled)


def draw_fronts(key, part):
    first_key, second_key = jax.random.split(jax.random.fold_in(key, 23))
    sample = jnp.clip(jax.random.normal(first_key, (LAYERS, NP, P_SIZE, P_SIZE), jnp.float32), -4.0, 4.0)
    symmetric = 2.5 * jnp.clip((sample + jnp.swapaxes(sample, -1, -2)) * 0.7071, -4.0, 4.0)
    diagonal = jax.random.uniform(second_key, (LAYERS, NP, P_SIZE), jnp.float32, 200.0, 360.0)
    is_diagonal = jnp.eye(P_SIZE, dtype=bool)
    return jnp.where(is_diagonal, diagonal[..., None], symmetric)


def place_ends(array, stream_key, low, largest):
    dims = array.shape
    place = [jax.random.randint(jax.random.fold_in(stream_key, axis), (), 0, dims[axis]) for axis in range(len(dims))]
    array = array.at[tuple(place)].set(low)
    longest = dims.index(max(dims))
    place[longest] = (place[longest] + 1) % dims[longest]
    return array.at[tuple(place)].set(largest)


def level_of(own_key, extent, pieces, least, top_value):
    level = 1.0
    for axis_at, shards_of in pieces:
        draws = jax.random.uniform(jax.random.fold_in(jax.random.fold_in(own_key, 6), axis_at), (shards_of,), jnp.float32, least / len(pieces), top_value / len(pieces))
        level = level * jnp.repeat(jnp.exp(draws), extent[axis_at] // shards_of).reshape((-1,) + (1,) * (len(extent) - 1 - axis_at))
    return level


def bell_draw(key, extent, deviation, limit, cuts=(), kind=jnp.bfloat16):
    drawn = deviation * jax.random.normal(key, extent, jnp.float32)
    if cuts:
        drawn = drawn * level_of(key, extent, cuts, -0.22, 0.18)
    return jnp.clip(drawn, -limit, limit).astype(kind)


def setup_inputs(seed: int = 0) -> dict:
    key_list = jax.random.split(jax.random.key(seed), 5)
    ancestor = draw_ancestor(jax.random.fold_in(key_list[4], 71), 0)
    coupling = bell_draw(key_list[1], (LAYERS, S, NP * P_SIZE), 2.5, 10.0, ((0, 2), (1, 16)))
    fronts = draw_fronts(jax.random.fold_in(key_list[4], 71), 0)
    tile_pattern = place_ends((jax.random.randint(key_list[3], (LAYERS, NP, TILES), 0, 4) < 3).astype(jnp.int32), jax.random.fold_in(key_list[3], 1), 0, 1)
    return dict(ancestor=ancestor, coupling=coupling, fronts=fronts, tile_pattern=tile_pattern)


def reference(ancestor, coupling, fronts, tile_pattern):
    front_chol = jnp.linalg.cholesky(fronts)
    tile_of_row = jnp.arange(S, dtype=jnp.int32) // TILE
    onehot = (tile_of_row[:, None] == jnp.arange(S // TILE, dtype=jnp.int32)[None, :]).astype(jnp.float32)
    schur = ancestor
    for layer_id in range(LAYERS):
        row_masks = jnp.dot(onehot, tile_pattern[layer_id].T.astype(jnp.float32))
        solved_parts = []
        for panel in range(NP):
            columns = coupling[layer_id, :, panel * P_SIZE:(panel + 1) * P_SIZE].astype(jnp.float32) * row_masks[:, panel:panel + 1]
            solved_parts.append(lax.linalg.triangular_solve(front_chol[layer_id, panel], columns, left_side=False, lower=True, transpose_a=True))
        scaled = jnp.concatenate(solved_parts, 1).astype(jnp.bfloat16)
        schur = schur - jnp.dot(scaled.astype(jnp.float32), scaled.T.astype(jnp.float32), preferred_element_type=jnp.float32)
    global_rows = jnp.arange(S, dtype=jnp.int32)
    panels = []
    pivot_list = []
    for section in range(ANC):
        offset = section * P_SIZE
        pivot_chol = jnp.linalg.cholesky(schur[offset:offset + P_SIZE, offset:offset + P_SIZE])
        solved = lax.linalg.triangular_solve(pivot_chol, schur[:, offset:offset + P_SIZE], left_side=False, lower=True, transpose_a=True)
        panel_rows = jnp.where((global_rows >= offset)[:, None], solved, jnp.zeros_like(solved))
        schur = schur - jnp.dot(panel_rows.astype(jnp.float32), panel_rows.T.astype(jnp.float32), precision=lax.Precision.HIGHEST, preferred_element_type=jnp.float32)
        panels.append(panel_rows)
        diagonal = jnp.diagonal(pivot_chol)
        pivot_list.append(diagonal * diagonal)
    return (schur, jnp.concatenate(panels, 1), jnp.concatenate(pivot_list))
```

```python
import functools

import jax
import jax.numpy as jnp
from jax import lax
from jax.experimental import pallas as pl
from jax.experimental.pallas import tpu as pltpu
from jax.sharding import PartitionSpec as P

TILE = 1024
P_SIZE = 512
NP = 2

BLOCK = 128
SUB = 8
GROUP = 4
HIGHEST = lax.Precision.HIGHEST


def eye_of(n, dtype=jnp.float32):
    return (
        lax.broadcasted_iota(jnp.int32, (n, n), 0) == lax.broadcasted_iota(jnp.int32, (n, n), 1)
    ).astype(dtype)


def eliminate(rows):
    count = len(rows)
    lanes = lax.broadcasted_iota(jnp.int32, (SUB, BLOCK), 1)
    subs = lax.broadcasted_iota(jnp.int32, (SUB, BLOCK), 0)
    rows = list(rows)
    ident = [(lanes == subs + SUB * i).astype(jnp.float32) for i in range(count)]

    def row_of(x, s):
        return jnp.broadcast_to(x[s : s + 1, :], (SUB, BLOCK))

    for base in range(0, BLOCK, GROUP):
        g, s = divmod(base, SUB)
        cols = [
            {i: jnp.broadcast_to(rows[i][:, base + t : base + t + 1], (SUB, BLOCK)) for i in range(g, count)}
            for t in range(GROUP)
        ]
        lead = [row_of(rows[g], s + t) for t in range(GROUP)]
        lead_id = [row_of(ident[g], s + t) for t in range(GROUP)]
        inverse = []
        for t in range(GROUP):
            inverse.append(1.0 / row_of(cols[t][g], s + t))
            for u in range(t + 1, GROUP):
                factor = row_of(cols[t][g], s + u) * inverse[t]
                lead[u] = lead[u] - factor * lead[t]
                lead_id[u] = lead_id[u] - factor * lead_id[t]
                for i in range(g, count):
                    cols[u][i] = cols[u][i] - cols[t][i] * factor
        lead_s = [lead[t] * inverse[t] for t in range(GROUP)]
        lead_is = [lead_id[t] * inverse[t] for t in range(GROUP)]
        for i in range(g, count):
            row, idn = rows[i], ident[i]
            for t in range(GROUP):
                m = cols[t][i]
                if i == g:
                    m = jnp.where(subs >= s + GROUP, m, 0.0)
                row = row - m * lead_s[t]
                idn = idn - m * lead_is[t]
            if i == g:
                for t in range(GROUP):
                    row = jnp.where(subs == s + t, lead[t], row)
                    idn = jnp.where(subs == s + t, lead_id[t], idn)
            rows[i], ident[i] = row, idn
    return rows, ident


def factor_kernel(a_ref, m_ref, t_ref, w_ref, d_ref, work):
    n = a_ref.shape[0]
    work[:, :n] = a_ref[...] - layer_dot(m_ref, t_ref)
    work[:, n:] = eye_of(n)
    lane = lax.broadcasted_iota(jnp.int32, (BLOCK, 2 * n), 1)

    def step(b, carry):
        first = pl.multiple_of(b * BLOCK, BLOCK)
        here = pl.ds(first, BLOCK)
        block = work[here, here]
        rows, ident = eliminate([block[SUB * i : SUB * (i + 1)] for i in range(BLOCK // SUB)])
        upper = jnp.concatenate(rows, 0)
        unit = jnp.concatenate(ident, 0)
        diag = eye_of(BLOCK) * upper
        pivots = jnp.sum(diag, axis=1, keepdims=True)
        d_ref[:, here] = jnp.broadcast_to(jnp.sum(diag, axis=0, keepdims=True), (SUB, BLOCK))
        small = unit * lax.rsqrt(pivots)
        lead = jnp.dot(small, work[here, :], precision=HIGHEST, preferred_element_type=jnp.float32)
        w_ref[here, :] = lead[:, n:]
        below = jnp.where(lane[:, :n] >= first + BLOCK, lead[:, :n], 0.0)
        work[...] -= lax.dot_general(
            below, lead, (((0,), (0,)), ((), ())), precision=HIGHEST, preferred_element_type=jnp.float32
        )
        return carry

    lax.fori_loop(0, n // BLOCK, step, 0)


def factor(block, lead_rows, lead_solved):
    n = block.shape[0]
    return pl.pallas_call(
        factor_kernel,
        out_shape=(
            jax.ShapeDtypeStruct((n, n), jnp.float32),
            jax.ShapeDtypeStruct((SUB, n), jnp.float32),
        ),
        in_specs=[pl.BlockSpec(memory_space=pltpu.VMEM)] * 3,
        out_specs=(pl.BlockSpec(memory_space=pltpu.VMEM),) * 2,
        scratch_shapes=[pltpu.VMEM((n, 2 * n), jnp.float32)],
        cost_estimate=pl.CostEstimate(flops=10**9 * 20, bytes_accessed=4 * n * n * 2, transcendentals=0),
        name="factor",
    )(block, lead_rows, lead_solved)


def inverse_kernel(f_ref, g_ref, x_ref, r_ref):
    n = f_ref.shape[0]
    f = f_ref[...]
    square = jnp.dot(f, f, preferred_element_type=jnp.float32)
    bound = jnp.sqrt(jnp.max(jnp.sum(jnp.abs(square), axis=1, keepdims=True), axis=0, keepdims=True))
    alpha = 1.7 / bound
    f32 = f.astype(jnp.float32)
    eye = eye_of(n)
    x_ref[...] = alpha * (2.0 * eye - alpha * f32)
    r_ref[...] = eye - alpha * (2.0 * f32 - alpha * square)

    def norm(r):
        return jnp.sum(r * r)

    def correct():
        return x_ref[...] + jnp.dot(
            x_ref[...].astype(jnp.bfloat16), r_ref[...].astype(jnp.bfloat16), preferred_element_type=jnp.float32
        )

    def body(state):
        count, _ = state
        x = correct()
        x_ref[...] = x
        high = x.astype(jnp.bfloat16)
        low = (x - high.astype(jnp.float32)).astype(jnp.bfloat16)
        r = (
            eye_of(n)
            - jnp.dot(f_ref[...], high, preferred_element_type=jnp.float32)
            - jnp.dot(f_ref[...], low, preferred_element_type=jnp.float32)
        )
        r_ref[...] = r
        return count + 1, norm(r)

    lax.while_loop(lambda state: (state[0] < 60) & (state[1] > 4e-4), body, (0, norm(r_ref[...])))
    g_ref[...] = correct().astype(g_ref.dtype)


def inverse(block):
    n = block.shape[0]
    return pl.pallas_call(
        inverse_kernel,
        out_shape=jax.ShapeDtypeStruct((n, n), jnp.bfloat16),
        in_specs=[pl.BlockSpec(memory_space=pltpu.VMEM)],
        out_specs=pl.BlockSpec(memory_space=pltpu.VMEM),
        scratch_shapes=[pltpu.VMEM((n, n), jnp.float32)] * 2,
        cost_estimate=pl.CostEstimate(flops=10**9 * 5, bytes_accessed=4 * n * n, transcendentals=0),
        name="inverse",
    )(block)


def dot32(a, b):
    return jnp.dot(a, b, preferred_element_type=jnp.float32)


def halves(x):
    high = x.astype(jnp.bfloat16)
    return high, (x - high.astype(jnp.float32)).astype(jnp.bfloat16)


def apply_kernel(g_ref, m_ref, t_ref):
    n = g_ref.shape[1]
    m = m_ref[0].reshape(t_ref.shape[1], n)
    t_ref[...] = lax.dot_general(
        g_ref[0], m, (((1,), (1,)), ((), ())), preferred_element_type=jnp.float32
    ).astype(t_ref.dtype)


def apply_inverse(inverses, rows):
    count, n, _ = inverses.shape
    layers, members, size, width = rows.shape
    panels = width // n
    tile = max(1, min(members, 1024 // size))
    return pl.pallas_call(
        apply_kernel,
        grid=(members // tile, count),
        in_specs=[
            pl.BlockSpec((1, n, n), lambda j, i: (i, 0, 0)),
            pl.BlockSpec((1, tile, size, n), lambda j, i: (i // panels, j, 0, i % panels)),
        ],
        out_specs=pl.BlockSpec((n, tile * size), lambda j, i: (i, j)),
        out_shape=jax.ShapeDtypeStruct((count * n, members * size), jnp.bfloat16),
        cost_estimate=pl.CostEstimate(
            flops=2 * count * n * n * members * size, bytes_accessed=4 * rows.size, transcendentals=0
        ),
        name="apply_inverse",
    )(inverses, rows)


def layer_dot(m_ref, t_ref):
    layers, members, size, width = m_ref.shape
    total = None
    for one in range(layers):
        part = dot32(m_ref[one].reshape(members * size, width), t_ref[one * width : (one + 1) * width])
        total = part if total is None else total + part
    return total


def row_panel_kernel(a_ref, m_ref, t_ref, w_ref, p_ref, high_ref, low_ref):
    s_high, s_low = halves(a_ref[...] - layer_dot(m_ref, t_ref))
    w_high, w_low = halves(w_ref[...].T)
    p = dot32(s_high, w_high) + dot32(s_high, w_low) + dot32(s_low, w_high)
    p_ref[...] = p
    high_ref[...], low_ref[...] = halves(p)


def row_panel(ancestor, rows, solved, weight):
    count, n = ancestor.shape
    layers, members, size, width = rows.shape
    deep = layers * width
    each = max(1, min(members, 512 // size))
    tile = each * size
    out = jax.ShapeDtypeStruct((count, n), jnp.bfloat16)
    spec = pl.BlockSpec((tile, n), lambda i: (i, 0))
    return pl.pallas_call(
        row_panel_kernel,
        grid=(count // tile,),
        in_specs=[
            spec,
            pl.BlockSpec((layers, each, size, width), lambda i: (0, i, 0, 0)),
            pl.BlockSpec((deep, n), lambda i: (0, 0)),
            pl.BlockSpec((n, n), lambda i: (0, 0)),
        ],
        out_specs=(spec, spec, spec),
        out_shape=(jax.ShapeDtypeStruct((count, n), jnp.float32), out, out),
        cost_estimate=pl.CostEstimate(
            flops=2 * count * n * (deep + 3 * n), bytes_accessed=2 * rows.size, transcendentals=0
        ),
        name="row_panel",
    )(ancestor, rows, solved, weight)


def col_panel_kernel(a_ref, m_ref, t_ref, w_ref, high_ref, low_ref):
    s_high, s_low = halves(a_ref[...] - layer_dot(m_ref, t_ref))
    w_high, w_low = halves(w_ref[...])
    high_ref[...], low_ref[...] = halves(dot32(w_high, s_high) + dot32(w_low, s_high) + dot32(w_high, s_low))


def col_panel(ancestor, lead, solved, weight):
    n, count = ancestor.shape
    tile = min(count, 512)
    deep = solved.shape[0]
    out = jax.ShapeDtypeStruct((n, count), jnp.bfloat16)
    spec = pl.BlockSpec((n, tile), lambda i: (0, i))
    return pl.pallas_call(
        col_panel_kernel,
        grid=(count // tile,),
        in_specs=[
            spec,
            pl.BlockSpec(lead.shape, lambda i: (0, 0, 0, 0)),
            pl.BlockSpec((deep, tile), lambda i: (0, i)),
            pl.BlockSpec((n, n), lambda i: (0, 0)),
        ],
        out_specs=(spec, spec),
        out_shape=(out, out),
        cost_estimate=pl.CostEstimate(
            flops=2 * count * n * (deep + 3 * n), bytes_accessed=2 * solved.size, transcendentals=0
        ),
        name="col_panel",
    )(ancestor, lead, solved, weight)


def schur_kernel(a_ref, m_ref, t_ref, ph_ref, pl_ref, qh_ref, ql_ref, out_ref):
    update = layer_dot(m_ref, t_ref)
    update += dot32(ph_ref[...], qh_ref[...])
    update += dot32(pl_ref[...], qh_ref[...])
    update += dot32(ph_ref[...], ql_ref[...])
    out_ref[...] = a_ref[...] - update


def schur_update(ancestor, rows, solved, p_high, p_low, q_high, q_low):
    height, width = ancestor.shape
    layers, members, size, each_width = rows.shape
    deep, n = layers * each_width, p_high.shape[1]
    each = max(1, min(members, 1024 // size))
    tall, wide = each * size, min(width, 512)
    block = pl.BlockSpec((tall, wide), lambda i, j: (i, j))
    p_spec = pl.BlockSpec((tall, n), lambda i, j: (i, 0))
    q_spec = pl.BlockSpec((n, wide), lambda i, j: (0, j))
    return pl.pallas_call(
        schur_kernel,
        grid=(height // tall, width // wide),
        in_specs=[
            block,
            pl.BlockSpec((layers, each, size, each_width), lambda i, j: (0, i, 0, 0)),
            pl.BlockSpec((deep, wide), lambda i, j: (0, j)),
            p_spec,
            p_spec,
            q_spec,
            q_spec,
        ],
        out_specs=block,
        out_shape=jax.ShapeDtypeStruct((height, width), jnp.float32),
        cost_estimate=pl.CostEstimate(
            flops=2 * height * width * (deep + 3 * n), bytes_accessed=8 * height * width, transcendentals=0
        ),
        name="schur_update",
    )(ancestor, rows, solved, p_high, p_low, q_high, q_low)


def shift(x, axis, step):
    n = lax.axis_size(axis)
    return lax.ppermute(x, axis, [(i, (i + step) % n) for i in range(n)])


def flip(x, axis, bit):
    n = lax.axis_size(axis)
    return lax.ppermute(x, axis, [(i, i ^ bit) for i in range(n)])


def put(buffer, x, *place):
    place = place + (0,) * (buffer.ndim - len(place))
    x = x.reshape((1,) * (buffer.ndim - x.ndim) + x.shape)
    return lax.dynamic_update_slice(buffer, x, tuple(jnp.int32(p) for p in place))


def layer_blocks(x):
    layers, here = lax.axis_size("layer"), lax.axis_index("layer")
    return [(x if s == 0 else shift(x, "layer", s), (here - s) % layers) for s in range(layers)]


def by_layer(x):
    stack = jnp.zeros((lax.axis_size("layer"),) + x.shape, x.dtype)
    for one, at in layer_blocks(x):
        stack = put(stack, one, at)
    return stack


def cube_blocks(x, axis):
    n, here = lax.axis_size(axis), lax.axis_index(axis)
    pieces = [(x, here)]
    bit = n // 2
    while bit:
        pieces += [(flip(p, axis, bit), at ^ bit) for p, at in pieces]
        bit //= 2
    return pieces


def spread_tree(x, axis):
    n, here = lax.axis_size(axis), lax.axis_index(axis)
    bit = n // 2
    while bit:
        got = lax.ppermute(x, axis, [(i, i ^ bit) for i in range(0, n, 2 * bit)])
        x = jnp.where((here & (2 * bit - 1)) == bit, got, x)
        bit //= 2
    return x


def spread_lead(x):
    n, here = lax.axis_size("col"), lax.axis_index("col")
    bit = n // 2
    while bit:
        got = lax.ppermute(x, ("row", "col"), [(i, i ^ bit) for i in range(0, n, 2 * bit)])
        x = jnp.where((here & (2 * bit - 1)) == bit, got, x)
        bit //= 2
    return spread_tree(x, "row")


def spread_line(x, axis, chunks):
    n, here = lax.axis_size(axis), lax.axis_index(axis)
    results = []
    for part in jnp.split(x, chunks, 0):
        result = got = part
        for d in range(1, n):
            got = lax.ppermute(got, axis, [(d - 1, d)])
            result = jnp.where(here == d, got, result)
        results.append(result)
    return jnp.concatenate(results, 0)


def local(ancestor, coupling, fronts, tile_pattern):
    layers, row_count, col_count = (lax.axis_size(a) for a in ("layer", "row", "col"))
    layer, row, col = (lax.axis_index(a) for a in ("layer", "row", "col"))
    local_rows, width = coupling.shape[1:]
    block_rows, block_cols = ancestor.shape

    first_row = (row * col_count + col) * local_rows
    tile = (first_row + lax.iota(jnp.int32, local_rows)) // TILE
    tiles = tile_pattern.shape[2]
    chosen = (tile[:, None] == lax.iota(jnp.int32, tiles)[None, :]).astype(jnp.float32)
    masks = jnp.dot(chosen, tile_pattern[0].T.astype(jnp.float32))
    masked = coupling[0] * jnp.repeat(masks, P_SIZE, axis=1).astype(coupling.dtype)

    panel = row % NP
    share = jnp.swapaxes(fronts[0], 1, 2).astype(jnp.bfloat16)
    share = lax.all_gather(share, "row", axis=0)
    share = lax.dynamic_index_in_dim(share, panel, 1, keepdims=False)
    share = lax.all_gather(share, "col", axis=0)
    front = jnp.swapaxes(share, 0, 1).reshape(P_SIZE, P_SIZE)
    own_inverse = inverse(front)

    pivot = spread_lead(ancestor[:P_SIZE, :P_SIZE])
    lead_fast = local_rows >= P_SIZE
    if lead_fast:
        lead_one = spread_lead(masked[:P_SIZE])
        lead = by_layer(lead_one)[:, None]

    masked, ancestor_in, _ = lax.optimization_barrier((masked, ancestor, front))

    own_pair = by_layer(own_inverse)
    inverses = jnp.zeros((layers, NP, P_SIZE, P_SIZE), jnp.bfloat16)
    for t in range(NP):
        pairs = [(i, i // NP * NP + (i + t) % NP) for i in range(row_count)]
        got = own_pair if t == 0 else lax.ppermute(own_pair, "row", pairs)
        inverses = put(inverses, got[:, None], 0, (panel - t) % NP)
    inverses = inverses.reshape(layers * NP, P_SIZE, P_SIZE)

    rows = jnp.zeros((layers, col_count, local_rows, width), jnp.bfloat16)
    for piece, at in cube_blocks(masked, "col"):
        for one, place in layer_blocks(piece):
            rows = put(rows, one, place, at)
    turned = lax.ppermute(
        masked,
        ("row", "col"),
        [(i * col_count + j, j * col_count + i) for i in range(row_count) for j in range(col_count)],
    )
    cols = jnp.zeros((layers, row_count, local_rows, width), jnp.bfloat16)
    for piece, at in cube_blocks(by_layer(turned), "row"):
        cols = put(cols, piece[:, None], 0, at)
    if not lead_fast:
        lead = spread_tree(rows[:, : P_SIZE // local_rows], "row")

    part = block_rows // layers
    left = lax.dynamic_slice_in_dim(ancestor_in[:, :P_SIZE], layer * part, part, 0)
    left = by_layer(spread_line(left, "col", 2)).reshape(block_rows, P_SIZE)
    top = spread_tree(ancestor_in[:P_SIZE], "row")

    lead_solved = apply_inverse(inverses, lead)
    weight, pivots = factor(pivot, lead, lead_solved)
    solved = apply_inverse(inverses, cols)
    p_full, p_high, p_low = row_panel(left, rows, lead_solved, weight)
    q_high, q_low = col_panel(top, lead, solved, weight)
    schur = schur_update(ancestor, rows, solved, p_high, p_low, q_high, q_low)
    panel_out = lax.dynamic_slice_in_dim(p_full, col * local_rows, local_rows, 0)
    share_size = P_SIZE // (row_count * col_count)
    my_pivots = lax.dynamic_slice_in_dim(pivots[0], (row * col_count + col) * share_size, share_size, 0)
    return schur, panel_out, my_pivots


def solution(mesh):
    return jax.shard_map(
        local,
        mesh=mesh,
        in_specs=(
            P("row", "col"),
            P("layer", ("row", "col"), None),
            P("layer", None, None, ("row", "col")),
            P("layer", None, None),
        ),
        out_specs=(P("row", "col"), P(("row", "col"), None), P(("row", "col"))),
        check_vma=False,
    )
```

```python
import functools

import jax
import jax.numpy as jnp
from jax import lax
from jax.experimental import pallas as pl
from jax.experimental.pallas import tpu as pltpu
from jax.sharding import PartitionSpec as P

TILE = 1024
P_SIZE = 512
NP = 2

BLOCK = 128
SUB = 8
GROUP = 4
HIGHEST = lax.Precision.HIGHEST


def eye_of(n, dtype=jnp.float32):
    return (
        lax.broadcasted_iota(jnp.int32, (n, n), 0) == lax.broadcasted_iota(jnp.int32, (n, n), 1)
    ).astype(dtype)


def eliminate(rows):
    count = len(rows)
    lanes = lax.broadcasted_iota(jnp.int32, (SUB, BLOCK), 1)
    subs = lax.broadcasted_iota(jnp.int32, (SUB, BLOCK), 0)
    rows = list(rows)
    ident = [(lanes == subs + SUB * i).astype(jnp.float32) for i in range(count)]

    def row_of(x, s):
        return jnp.broadcast_to(x[s : s + 1, :], (SUB, BLOCK))

    for base in range(0, BLOCK, GROUP):
        g, s = divmod(base, SUB)
        cols = [
            {i: jnp.broadcast_to(rows[i][:, base + t : base + t + 1], (SUB, BLOCK)) for i in range(g, count)}
            for t in range(GROUP)
        ]
        lead = [row_of(rows[g], s + t) for t in range(GROUP)]
        lead_id = [row_of(ident[g], s + t) for t in range(GROUP)]
        inverse = []
        for t in range(GROUP):
            inverse.append(1.0 / row_of(cols[t][g], s + t))
            for u in range(t + 1, GROUP):
                factor = row_of(cols[t][g], s + u) * inverse[t]
                lead[u] = lead[u] - factor * lead[t]
                lead_id[u] = lead_id[u] - factor * lead_id[t]
                for i in range(g, count):
                    cols[u][i] = cols[u][i] - cols[t][i] * factor
        lead_s = [lead[t] * inverse[t] for t in range(GROUP)]
        lead_is = [lead_id[t] * inverse[t] for t in range(GROUP)]
        for i in range(g, count):
            row, idn = rows[i], ident[i]
            for t in range(GROUP):
                m = cols[t][i]
                if i == g:
                    m = jnp.where(subs >= s + GROUP, m, 0.0)
                row = row - m * lead_s[t]
                idn = idn - m * lead_is[t]
            if i == g:
                for t in range(GROUP):
                    row = jnp.where(subs == s + t, lead[t], row)
                    idn = jnp.where(subs == s + t, lead_id[t], idn)
            rows[i], ident[i] = row, idn
    return rows, ident


def factor_kernel(a_ref, m_ref, t_ref, w_ref, d_ref, work):
    n = a_ref.shape[0]
    work[:, :n] = a_ref[...] - layer_dot(m_ref, t_ref)
    work[:, n:] = eye_of(n)
    lane = lax.broadcasted_iota(jnp.int32, (BLOCK, 2 * n), 1)

    def step(b, carry):
        first = pl.multiple_of(b * BLOCK, BLOCK)
        here = pl.ds(first, BLOCK)
        block = work[here, here]
        rows, ident = eliminate([block[SUB * i : SUB * (i + 1)] for i in range(BLOCK // SUB)])
        upper = jnp.concatenate(rows, 0)
        unit = jnp.concatenate(ident, 0)
        diag = eye_of(BLOCK) * upper
        pivots = jnp.sum(diag, axis=1, keepdims=True)
        d_ref[:, here] = jnp.broadcast_to(jnp.sum(diag, axis=0, keepdims=True), (SUB, BLOCK))
        small = unit * lax.rsqrt(pivots)
        lead = jnp.dot(small, work[here, :], precision=HIGHEST, preferred_element_type=jnp.float32)
        w_ref[here, :] = lead[:, n:]
        below = jnp.where(lane[:, :n] >= first + BLOCK, lead[:, :n], 0.0)
        work[...] -= lax.dot_general(
            below, lead, (((0,), (0,)), ((), ())), precision=HIGHEST, preferred_element_type=jnp.float32
        )
        return carry

    lax.fori_loop(0, n // BLOCK, step, 0)


def factor(block, lead_rows, lead_solved):
    n = block.shape[0]
    return pl.pallas_call(
        factor_kernel,
        out_shape=(
            jax.ShapeDtypeStruct((n, n), jnp.float32),
            jax.ShapeDtypeStruct((SUB, n), jnp.float32),
        ),
        in_specs=[pl.BlockSpec(memory_space=pltpu.VMEM)] * 3,
        out_specs=(pl.BlockSpec(memory_space=pltpu.VMEM),) * 2,
        scratch_shapes=[pltpu.VMEM((n, 2 * n), jnp.float32)],
        cost_estimate=pl.CostEstimate(flops=10**9 * 20, bytes_accessed=4 * n * n * 2, transcendentals=0),
        name="factor",
    )(block, lead_rows, lead_solved)


def inverse_kernel(f_ref, g_ref, x_ref, r_ref):
    n = f_ref.shape[0]
    f = f_ref[...]
    square = jnp.dot(f, f, preferred_element_type=jnp.float32)
    bound = jnp.sqrt(jnp.max(jnp.sum(jnp.abs(square), axis=1, keepdims=True), axis=0, keepdims=True))
    alpha = 1.7 / bound
    f32 = f.astype(jnp.float32)
    eye = eye_of(n)
    x_ref[...] = alpha * (2.0 * eye - alpha * f32)
    r_ref[...] = eye - alpha * (2.0 * f32 - alpha * square)

    def norm(r):
        return jnp.sum(r * r)

    def correct():
        return x_ref[...] + jnp.dot(
            x_ref[...].astype(jnp.bfloat16), r_ref[...].astype(jnp.bfloat16), preferred_element_type=jnp.float32
        )

    def body(state):
        count, _ = state
        x = correct()
        x_ref[...] = x
        high = x.astype(jnp.bfloat16)
        low = (x - high.astype(jnp.float32)).astype(jnp.bfloat16)
        r = (
            eye_of(n)
            - jnp.dot(f_ref[...], high, preferred_element_type=jnp.float32)
            - jnp.dot(f_ref[...], low, preferred_element_type=jnp.float32)
        )
        r_ref[...] = r
        return count + 1, norm(r)

    lax.while_loop(lambda state: (state[0] < 60) & (state[1] > 4e-4), body, (0, norm(r_ref[...])))
    g_ref[...] = correct().astype(g_ref.dtype)


def inverse(block):
    n = block.shape[0]
    return pl.pallas_call(
        inverse_kernel,
        out_shape=jax.ShapeDtypeStruct((n, n), jnp.bfloat16),
        in_specs=[pl.BlockSpec(memory_space=pltpu.VMEM)],
        out_specs=pl.BlockSpec(memory_space=pltpu.VMEM),
        scratch_shapes=[pltpu.VMEM((n, n), jnp.float32)] * 2,
        cost_estimate=pl.CostEstimate(flops=10**9 * 5, bytes_accessed=4 * n * n, transcendentals=0),
        name="inverse",
    )(block)


def dot32(a, b):
    return jnp.dot(a, b, preferred_element_type=jnp.float32)


def halves(x):
    high = x.astype(jnp.bfloat16)
    return high, (x - high.astype(jnp.float32)).astype(jnp.bfloat16)


def apply_kernel(g_ref, m_ref, t_ref):
    n = g_ref.shape[1]
    m = m_ref[0].reshape(t_ref.shape[1], n)
    t_ref[...] = lax.dot_general(
        g_ref[0], m, (((1,), (1,)), ((), ())), preferred_element_type=jnp.float32
    ).astype(t_ref.dtype)


def apply_inverse(inverses, rows):
    count, n, _ = inverses.shape
    layers, members, size, width = rows.shape
    panels = width // n
    tile = max(1, min(members, 1024 // size))
    return pl.pallas_call(
        apply_kernel,
        grid=(members // tile, count),
        in_specs=[
            pl.BlockSpec((1, n, n), lambda j, i: (i, 0, 0)),
            pl.BlockSpec((1, tile, size, n), lambda j, i: (i // panels, j, 0, i % panels)),
        ],
        out_specs=pl.BlockSpec((n, tile * size), lambda j, i: (i, j)),
        out_shape=jax.ShapeDtypeStruct((count * n, members * size), jnp.bfloat16),
        cost_estimate=pl.CostEstimate(
            flops=2 * count * n * n * members * size, bytes_accessed=4 * rows.size, transcendentals=0
        ),
        name="apply_inverse",
    )(inverses, rows)


def layer_dot(m_ref, t_ref):
    layers, members, size, width = m_ref.shape
    total = None
    for one in range(layers):
        part = dot32(m_ref[one].reshape(members * size, width), t_ref[one * width : (one + 1) * width])
        total = part if total is None else total + part
    return total


def row_panel_kernel(a_ref, m_ref, t_ref, w_ref, p_ref, high_ref, low_ref):
    s_high, s_low = halves(a_ref[...] - layer_dot(m_ref, t_ref))
    w_high, w_low = halves(w_ref[...].T)
    p = dot32(s_high, w_high) + dot32(s_high, w_low) + dot32(s_low, w_high)
    p_ref[...] = p
    high_ref[...], low_ref[...] = halves(p)


def row_panel(ancestor, rows, solved, weight):
    count, n = ancestor.shape
    layers, members, size, width = rows.shape
    deep = layers * width
    each = max(1, min(members, 512 // size))
    tile = each * size
    out = jax.ShapeDtypeStruct((count, n), jnp.bfloat16)
    spec = pl.BlockSpec((tile, n), lambda i: (i, 0))
    return pl.pallas_call(
        row_panel_kernel,
        grid=(count // tile,),
        in_specs=[
            spec,
            pl.BlockSpec((layers, each, size, width), lambda i: (0, i, 0, 0)),
            pl.BlockSpec((deep, n), lambda i: (0, 0)),
            pl.BlockSpec((n, n), lambda i: (0, 0)),
        ],
        out_specs=(spec, spec, spec),
        out_shape=(jax.ShapeDtypeStruct((count, n), jnp.float32), out, out),
        cost_estimate=pl.CostEstimate(
            flops=2 * count * n * (deep + 3 * n), bytes_accessed=2 * rows.size, transcendentals=0
        ),
        name="row_panel",
    )(ancestor, rows, solved, weight)


def col_panel_kernel(a_ref, m_ref, t_ref, w_ref, high_ref, low_ref):
    s_high, s_low = halves(a_ref[...] - layer_dot(m_ref, t_ref))
    w_high, w_low = halves(w_ref[...])
    high_ref[...], low_ref[...] = halves(dot32(w_high, s_high) + dot32(w_low, s_high) + dot32(w_high, s_low))


def col_panel(ancestor, lead, solved, weight):
    n, count = ancestor.shape
    tile = min(count, 512)
    deep = solved.shape[0]
    out = jax.ShapeDtypeStruct((n, count), jnp.bfloat16)
    spec = pl.BlockSpec((n, tile), lambda i: (0, i))
    return pl.pallas_call(
        col_panel_kernel,
        grid=(count // tile,),
        in_specs=[
            spec,
            pl.BlockSpec(lead.shape, lambda i: (0, 0, 0, 0)),
            pl.BlockSpec((deep, tile), lambda i: (0, i)),
            pl.BlockSpec((n, n), lambda i: (0, 0)),
        ],
        out_specs=(spec, spec),
        out_shape=(out, out),
        cost_estimate=pl.CostEstimate(
            flops=2 * count * n * (deep + 3 * n), bytes_accessed=2 * solved.size, transcendentals=0
        ),
        name="col_panel",
    )(ancestor, lead, solved, weight)


def schur_kernel(a_ref, m_ref, t_ref, ph_ref, pl_ref, qh_ref, ql_ref, out_ref):
    update = layer_dot(m_ref, t_ref)
    update += dot32(ph_ref[...], qh_ref[...])
    update += dot32(pl_ref[...], qh_ref[...])
    update += dot32(ph_ref[...], ql_ref[...])
    out_ref[...] = a_ref[...] - update


def schur_update(ancestor, rows, solved, p_high, p_low, q_high, q_low):
    height, width = ancestor.shape
    layers, members, size, each_width = rows.shape
    deep, n = layers * each_width, p_high.shape[1]
    each = max(1, min(members, 1024 // size))
    tall, wide = each * size, min(width, 512)
    block = pl.BlockSpec((tall, wide), lambda i, j: (i, j))
    p_spec = pl.BlockSpec((tall, n), lambda i, j: (i, 0))
    q_spec = pl.BlockSpec((n, wide), lambda i, j: (0, j))
    return pl.pallas_call(
        schur_kernel,
        grid=(height // tall, width // wide),
        in_specs=[
            block,
            pl.BlockSpec((layers, each, size, each_width), lambda i, j: (0, i, 0, 0)),
            pl.BlockSpec((deep, wide), lambda i, j: (0, j)),
            p_spec,
            p_spec,
            q_spec,
            q_spec,
        ],
        out_specs=block,
        out_shape=jax.ShapeDtypeStruct((height, width), jnp.float32),
        cost_estimate=pl.CostEstimate(
            flops=2 * height * width * (deep + 3 * n), bytes_accessed=8 * height * width, transcendentals=0
        ),
        name="schur_update",
    )(ancestor, rows, solved, p_high, p_low, q_high, q_low)


def shift(x, axis, step):
    n = lax.axis_size(axis)
    return lax.ppermute(x, axis, [(i, (i + step) % n) for i in range(n)])


def flip(x, axis, bit):
    n = lax.axis_size(axis)
    return lax.ppermute(x, axis, [(i, i ^ bit) for i in range(n)])


def put(buffer, x, *place):
    place = place + (0,) * (buffer.ndim - len(place))
    x = x.reshape((1,) * (buffer.ndim - x.ndim) + x.shape)
    return lax.dynamic_update_slice(buffer, x, tuple(jnp.int32(p) for p in place))


def layer_blocks(x):
    layers, here = lax.axis_size("layer"), lax.axis_index("layer")
    return [(x if s == 0 else shift(x, "layer", s), (here - s) % layers) for s in range(layers)]


def by_layer(x):
    stack = jnp.zeros((lax.axis_size("layer"),) + x.shape, x.dtype)
    for one, at in layer_blocks(x):
        stack = put(stack, one, at)
    return stack


def cube_blocks(x, axis):
    n, here = lax.axis_size(axis), lax.axis_index(axis)
    pieces = [(x, here)]
    bit = n // 2
    while bit:
        pieces += [(flip(p, axis, bit), at ^ bit) for p, at in pieces]
        bit //= 2
    return pieces


def spread_tree(x, axis):
    n, here = lax.axis_size(axis), lax.axis_index(axis)
    bit = n // 2
    while bit:
        got = lax.ppermute(x, axis, [(i, i ^ bit) for i in range(0, n, 2 * bit)])
        x = jnp.where((here & (2 * bit - 1)) == bit, got, x)
        bit //= 2
    return x


def spread_first(x):
    n, here = lax.axis_size("col"), lax.axis_index("col")
    bit = n // 2
    while bit:
        got = lax.ppermute(x, ("row", "col"), [(i, i ^ bit) for i in range(0, n, 2 * bit)])
        x = jnp.where((here & (2 * bit - 1)) == bit, got, x)
        bit //= 2
    return x


def spread_line(x, axis, chunks):
    n, here = lax.axis_size(axis), lax.axis_index(axis)
    results = []
    for part in jnp.split(x, chunks, 0):
        result = got = part
        for d in range(1, n):
            got = lax.ppermute(got, axis, [(d - 1, d)])
            result = jnp.where(here == d, got, result)
        results.append(result)
    return jnp.concatenate(results, 0)


def local(ancestor, coupling, fronts, tile_pattern):
    layers, row_count, col_count = (lax.axis_size(a) for a in ("layer", "row", "col"))
    layer, row, col = (lax.axis_index(a) for a in ("layer", "row", "col"))
    local_rows, width = coupling.shape[1:]
    block_rows, block_cols = ancestor.shape

    first_row = (row * col_count + col) * local_rows
    tile = (first_row + lax.iota(jnp.int32, local_rows)) // TILE
    tiles = tile_pattern.shape[2]
    chosen = (tile[:, None] == lax.iota(jnp.int32, tiles)[None, :]).astype(jnp.float32)
    masks = jnp.dot(chosen, tile_pattern[0].T.astype(jnp.float32))
    masked = coupling[0] * jnp.repeat(masks, P_SIZE, axis=1).astype(coupling.dtype)

    panel = row % NP
    share = jnp.swapaxes(fronts[0], 1, 2).astype(jnp.bfloat16)
    share = lax.all_gather(share, "row", axis=0)
    share = lax.dynamic_index_in_dim(share, panel, 1, keepdims=False)
    share = lax.all_gather(share, "col", axis=0)
    front = jnp.swapaxes(share, 0, 1).reshape(P_SIZE, P_SIZE)
    own_inverse = inverse(front)

    pivot = first_pivot = spread_first(ancestor[:P_SIZE, :P_SIZE])
    lead_fast = local_rows >= P_SIZE
    if lead_fast:
        first_lead = spread_first(masked[:P_SIZE])
        lead = by_layer(spread_tree(first_lead, "row"))[:, None]
    else:
        first_lead = first_pivot
    pivot = spread_tree(pivot, "row")

    masked, ancestor_in, _ = lax.optimization_barrier((masked, ancestor, front))
    later, left, _, _ = lax.optimization_barrier((masked, ancestor_in[:, :P_SIZE], first_pivot, first_lead))

    own_pair = by_layer(own_inverse)
    inverses = jnp.zeros((layers, NP, P_SIZE, P_SIZE), jnp.bfloat16)
    for t in range(NP):
        pairs = [(i, i // NP * NP + (i + t) % NP) for i in range(row_count)]
        got = own_pair if t == 0 else lax.ppermute(own_pair, "row", pairs)
        inverses = put(inverses, got[:, None], 0, (panel - t) % NP)
    inverses = inverses.reshape(layers * NP, P_SIZE, P_SIZE)

    rows = jnp.zeros((layers, col_count, local_rows, width), jnp.bfloat16)
    for piece, at in cube_blocks(masked, "col"):
        for one, place in layer_blocks(piece):
            rows = put(rows, one, place, at)
    turned = lax.ppermute(
        later,
        ("row", "col"),
        [(i * col_count + j, j * col_count + i) for i in range(row_count) for j in range(col_count)],
    )
    cols = jnp.zeros((layers, row_count, local_rows, width), jnp.bfloat16)
    for piece, at in cube_blocks(by_layer(turned), "row"):
        cols = put(cols, piece[:, None], 0, at)
    if not lead_fast:
        lead = spread_tree(rows[:, : P_SIZE // local_rows], "row")

    part = block_rows // layers
    left = lax.dynamic_slice_in_dim(left, layer * part, part, 0)
    left = by_layer(spread_line(left, "col", 2)).reshape(block_rows, P_SIZE)
    top = spread_tree(ancestor_in[:P_SIZE], "row")

    lead_solved = apply_inverse(inverses, lead)
    weight, pivots = factor(pivot, lead, lead_solved)
    solved = apply_inverse(inverses, cols)
    p_full, p_high, p_low = row_panel(left, rows, lead_solved, weight)
    q_high, q_low = col_panel(top, lead, solved, weight)
    schur = schur_update(ancestor, rows, solved, p_high, p_low, q_high, q_low)
    panel_out = lax.dynamic_slice_in_dim(p_full, col * local_rows, local_rows, 0)
    share_size = P_SIZE // (row_count * col_count)
    my_pivots = lax.dynamic_slice_in_dim(pivots[0], (row * col_count + col) * share_size, share_size, 0)
    return schur, panel_out, my_pivots


def solution(mesh):
    return jax.shard_map(
        local,
        mesh=mesh,
        in_specs=(
            P("row", "col"),
            P("layer", ("row", "col"), None),
            P("layer", None, None, ("row", "col")),
            P("layer", None, None),
        ),
        out_specs=(P("row", "col"), P(("row", "col"), None), P(("row", "col"))),
        check_vma=False,
    )
```
